32 devices in a mesh: shear: 16 (over z, y, x), cross: 2 (over core).
Axes of the slice: x: 2, y: 2, z: 4, core: 2. Of those that a mesh axis runs over, the one named last changes fastest.
Arguments:
- positions: float32 [3, 16, 16, 2, 256], P(None, 'shear', None, 'cross'), may hold values from 0 to 1
- masses: float32 [16, 16, 2, 256], P('shear', None, 'cross'), may hold values from 0.002 to 0.008
- counts: int32 [16, 16, 2], P('shear', None, 'cross'), may hold values from 32 to 256
- shear_offset: int32 [1], replicated, may hold values from 0 to 15
Outputs:
- density: float32 [16, 16, 2, 256], P('shear', None, 'cross')
The draws below stay inside these ranges and needn't reach their ends.
Inputs may be any that keep to these rules, and one draw needn't show every extreme that they name: `shear_offset`: a whole number of cells.
All inputs are finite; a program needn't handle non-finite values.
Results may differ from the reference program's by a relative error of at most 0.0003.
Values sent between devices are 32-bit elements; how exact they have to be, the bound alone decides.
A program may use at most 64 MiB of HBM per device.

```python
import math
import jax
import jax.numpy as jnp
from jax import lax

P_SIZE = 256
NX = 16
NY = 16
NZ = 2


def place_ends(entries, stream_key, least, largest):
    index_at = [jax.random.randint(jax.random.fold_in(stream_key, axis), (), 0, length) for axis, length in enumerate(entries.shape)]
    main_axis = entries.shape.index(max(entries.shape))
    next_to = index_at[:main_axis] + [(index_at[main_axis] + 1) % entries.shape[main_axis]] + index_at[main_axis + 1:]
    return entries.at[tuple(index_at)].set(least).at[tuple(next_to)].set(largest)


def level_of(own_key, dims, pieces, least, largest):
    level = 1.0
    for position, blocks in pieces:
        heights = jax.random.uniform(jax.random.fold_in(jax.random.fold_in(own_key, 6), position), (blocks,), jnp.float32, least / len(pieces), largest / len(pieces))
        level = level * jnp.repeat(jnp.exp(heights), dims[position] // blocks).reshape((-1,) + (1,) * (len(dims) - 1 - position))
    return level


def setup_inputs(seed: int = 0) -> dict:
    splits = jax.random.split(jax.random.key(seed), 5)
    positions = jnp.clip(1.0 * jax.random.uniform(splits[0], (3, NY, NX, NZ, P_SIZE), jnp.float32) ** level_of(splits[0], (3, NY, NX, NZ, P_SIZE), ((1, 16), (3, 2)), -0.2, 0.2), 0.0, 1.0)
    masses = jnp.clip(jnp.exp(math.log(0.008) - 1.3862944 * jax.random.uniform(splits[1], (NY, NX, NZ, P_SIZE), jnp.float32) ** level_of(splits[1], (NY, NX, NZ, P_SIZE), ((0, 16), (2, 2)), -0.2, 0.2)), 0.002, 0.008)
    counts = place_ends(jax.random.randint(splits[2], (NY, NX, NZ), P_SIZE // 8, P_SIZE + 1), jax.random.fold_in(splits[2], 1), P_SIZE // 8, P_SIZE).astype(jnp.int32)
    shear_offset = jax.random.randint(splits[3], (1,), 0, NX).astype(jnp.int32)
    return dict(positions=positions, masses=masses, counts=counts, shear_offset=shear_offset)


def spline(squared):
    radius = jnp.sqrt(squared) * 4.0
    inner_part = 1.0 - 1.5 * radius * radius + 0.75 * radius * radius * radius
    outer_part = 0.25 * jnp.maximum(2.0 - radius, 0.0) ** 3
    return jnp.where(radius < 1.0, inner_part, outer_part) * (64.0 / 3.141592653589793)

def distance_sq(target, source_pos, offset_vec):
    squared = None
    for component in range(3):
        moved = source_pos[component] + offset_vec[component]
        gap = target[component][..., :, None] - moved[..., None, :]
        squared = gap * gap if squared is None else squared + gap * gap
    return squared

def reference(positions, masses, counts, shear_offset):
    slot_index = lax.broadcasted_iota(jnp.int32, masses.shape, 3)
    is_valid = slot_index < counts[..., None]
    weight = jnp.where(is_valid, masses, jnp.float32(0.0))
    particle_data = jnp.concatenate([positions, weight[None]], 0)
    offset = shear_offset[0]
    top_row = jnp.roll(particle_data[:, 0:1], -offset, axis=2)
    bottom_row = jnp.roll(particle_data[:, -1:], offset, axis=2)
    extended = jnp.concatenate([bottom_row, particle_data, top_row], 1)
    extended = jnp.concatenate([extended[:, :, :, -1:], extended, extended[:, :, :, :1]], 3)
    width_z = masses.shape[2]

    def row_density(row_at):
        band = lax.dynamic_slice_in_dim(extended, row_at, 3, 1)
        target = band[:3, 1, :, 1:1 + width_z]
        density = jnp.zeros(target.shape[1:], jnp.float32)
        for step_y in (-1, 0, 1):
            for step_z in (-1, 0, 1):
                for step_x in (-1, 0, 1):
                    source_cells = jnp.roll(band[:, 1 + step_y, :, 1 + step_z:1 + step_z + width_z], -step_x, axis=1)
                    offset_vec = (float(step_y), float(step_x), float(step_z))
                    kernel = spline(distance_sq(target, source_cells[:3], offset_vec))
                    density = density + lax.optimization_barrier(jnp.sum(kernel * source_cells[3][..., None, :], axis=-1))
        valid_row = lax.dynamic_index_in_dim(is_valid, row_at, 0, keepdims=False)
        return jnp.where(valid_row, density, jnp.float32(0.0))
    return lax.map(row_density, jnp.arange(masses.shape[0], dtype=jnp.int32))
```

```python
import functools
import jax
import jax.numpy as jnp
from jax import lax
from jax.experimental import pallas as pl
from jax.experimental.pallas import tpu as pltpu
from jax.sharding import PartitionSpec as P

BLOCK = 16
PER_CHUNK = 8
FEATURES = 32


def extended_2(block, sides, width):
    for axis, dim in sides:
        count = lax.axis_size(axis)
        forward = [(i, (i + 1) % count) for i in range(count)]
        backward = [(target, source) for source, target in forward]
        low = lax.ppermute(
            lax.slice_in_dim(block, block.shape[dim] - width, None, axis=dim), axis, forward
        )
        high = lax.ppermute(lax.slice_in_dim(block, 0, width, axis=dim), axis, backward)
        block = jnp.concatenate([low, block, high], axis=dim)
    return block


def split3(x):
    high = lax.reduce_precision(x, 8, 7)
    rest = x - high
    middle = lax.reduce_precision(rest, 8, 7)
    low = lax.reduce_precision(rest - middle, 8, 7)
    return high, middle, low


def source_rows(coords, weight):
    rows = []
    for value in coords:
        high, middle, low = split3(value)
        rows += [high, high, high, middle, middle, low]
    norm = coords[0] * coords[0] + coords[1] * coords[1] + coords[2] * coords[2]
    one = jnp.ones_like(norm)
    zero = jnp.zeros_like(norm)
    rows += list(split3(norm)) + [one] * 3 + list(split3(weight))
    rows += [zero] * (FEATURES - len(rows))
    return jnp.stack(rows, axis=-2).astype(jnp.bfloat16)


def target_rows(coords):
    rows = []
    for value in coords:
        high, middle, low = split3(-2.0 * value)
        rows += [high, middle, low, high, middle, high]
    norm = coords[0] * coords[0] + coords[1] * coords[1] + coords[2] * coords[2]
    one = jnp.ones_like(norm)
    zero = jnp.zeros_like(norm)
    rows += [one] * 3 + list(split3(norm))
    rows += [zero] * (FEATURES - len(rows))
    return jnp.stack(rows, axis=-2).astype(jnp.bfloat16)


def density_kernel(
    rooms, list_ref, chunks_ref, counts_ref, pos_ref, feat_ref, target_ref, out_ref,
    store_ref, lhs_a, lhs_b, sq_a, sq_b,
):
    cells, slots = out_ref.shape
    pairs = pos_ref.shape[0]
    unroll = 4
    zero_block = pairs * 2 * rooms
    store_ref[zero_block] = jnp.zeros((BLOCK, 128), jnp.bfloat16)
    row_id = lax.broadcasted_iota(jnp.int32, (rooms * BLOCK, slots), 0)

    def compact(step, carry):
        for k in range(unroll):
            pair = step * unroll + k
            chosen = jnp.where(row_id == pos_ref[pair], 1.0, 0.0).astype(jnp.bfloat16)
            for variant in range(2):
                rows = lax.dot_general(
                    chosen, feat_ref[pair, variant], (((1,), (1,)), ((), ())),
                    preferred_element_type=jnp.float32,
                )
                rows = jnp.concatenate(
                    [rows, jnp.zeros((rooms * BLOCK, 128 - FEATURES), jnp.float32)], axis=1
                )
                store_ref[pl.ds((pair * 2 + variant) * rooms, rooms)] = rows.astype(
                    jnp.bfloat16
                ).reshape(rooms, BLOCK, 128)
        return carry

    lax.fori_loop(0, pairs // unroll, compact, 0)

    mass_rows = lax.broadcasted_iota(jnp.int32, (FEATURES, 128), 0)
    spread = jnp.where((mass_rows >= 24) & (mass_rows < 27), 1.0, 0.0).astype(jnp.bfloat16)
    pad = jnp.zeros((128 - FEATURES, slots + 128), jnp.bfloat16)

    def cell_body(cell, carry):
        weights = jnp.concatenate([target_ref[cell], spread], axis=1)
        weights = jnp.concatenate([weights, pad], axis=0)

        def produce(chunk, sq_ref):
            blocks = [
                store_ref[list_ref[cell, chunk * PER_CHUNK + k]] for k in range(PER_CHUNK)
            ]
            lhs = jnp.concatenate(blocks, axis=0)
            sq_ref[...] = jnp.dot(lhs, weights, preferred_element_type=jnp.float32)

        def consume(sq_ref, acc):
            for group in range(PER_CHUNK * BLOCK // 8):
                rows = pl.ds(group * 8, 8)
                squared = jnp.maximum(sq_ref[rows, :slots], 1e-30)
                mass = sq_ref[rows, slots:]
                mass = jnp.concatenate([mass] * (slots // 128), axis=1)
                q = squared * lax.rsqrt(squared)
                outer = jnp.maximum(2.0 - q, 0.0)
                inner = jnp.maximum(outer - 1.0, 0.0)
                value = outer * outer * outer - 4.0 * (inner * inner * inner)
                acc = acc + mass * value
            return acc

        produce(0, sq_a)

        def pair_body(step, acc):
            produce(2 * step + 1, sq_b)
            acc = consume(sq_a, acc)
            produce(2 * step + 2, sq_a)
            return consume(sq_b, acc)

        acc = lax.fori_loop(
            0, (chunks_ref[cell] + 1) // 2, pair_body, jnp.zeros((8, slots), jnp.float32)
        )
        total = jnp.sum(acc, axis=0, keepdims=True) * (16.0 / 3.141592653589793)
        slot = lax.broadcasted_iota(jnp.int32, (1, slots), 1)
        out_ref[pl.ds(cell, 1), :] = jnp.where(slot < counts_ref[cell], total, 0.0)
        return carry

    lax.fori_loop(0, cells, cell_body, 0)


def shards(positions, masses, counts, shear_offset):
    cells_y, cells, cells_z, slots = masses.shape
    assert cells_y == 1 and cells_z == 1
    rooms = slots // BLOCK + 1
    slot_index = lax.broadcasted_iota(jnp.int32, masses.shape, 3)
    weight = jnp.where(slot_index < counts[..., None], masses, jnp.float32(0.0))
    data = jnp.concatenate([positions, weight[None]], 0)
    offset = shear_offset[0]
    shear_index = lax.axis_index("shear")
    cycle = lax.axis_size("shear")
    padded = extended_2(data, (("shear", 1), ("cross", 3)), 1)
    low_shift = jnp.where(shear_index == 0, -offset, 0)
    high_shift = jnp.where(shear_index == cycle - 1, offset, 0)

    features, masks, shifts = [], [], []
    for step_y in (-1, 0, 1):
        for step_z in (-1, 0, 1):
            y, x, z, mass = (padded[k, 1 + step_y, :, 1 + step_z] for k in range(4))
            keep = mass > 0.0
            for value, step in ((y, step_y), (z, step_z)):
                if step == -1:
                    keep = keep & (value >= 0.5)
                elif step == 1:
                    keep = keep & (value <= 0.5)
            lower = x <= 0.5
            masks.append(jnp.stack([keep & lower, keep & ~lower], 0))
            moved = jnp.where(lower, x + 1.0, x - 1.0)
            scaled_y = 4.0 * (y + (step_y - 0.5))
            scaled_z = 4.0 * (z + (step_z - 0.5))
            features.append(
                jnp.stack(
                    [
                        source_rows((scaled_y, 4.0 * (value - 0.5), scaled_z), mass)
                        for value in (x, moved)
                    ],
                    1,
                )
            )
            shifts.append({-1: low_shift, 0: jnp.int32(0), 1: high_shift}[step_y])
    features = jnp.concatenate(features, 0)
    chosen = jnp.stack(masks, 0)
    triangle = (
        lax.broadcasted_iota(jnp.int32, (slots, slots), 0)
        <= lax.broadcasted_iota(jnp.int32, (slots, slots), 1)
    ).astype(jnp.bfloat16)
    ranks = jnp.dot(
        chosen.reshape(-1, slots).astype(jnp.bfloat16), triangle,
        preferred_element_type=jnp.float32,
    ).astype(jnp.int32).reshape(chosen.shape)
    sizes = ranks[..., -1]
    blocks = (sizes + (BLOCK - 1)) // BLOCK
    pos = jnp.where(
        chosen[:, 0],
        ranks[:, 0] - 1,
        jnp.where(chosen[:, 1], ranks[:, 1] - 1 + BLOCK * blocks[:, 0, :, None], -1),
    ).reshape(-1, 1, slots)

    relations = len(masks)
    shift = jnp.stack(shifts)
    target = lax.broadcasted_iota(jnp.int32, (cells, relations, 3), 0)
    relation = lax.broadcasted_iota(jnp.int32, (cells, relations, 3), 1)
    step_x = lax.broadcasted_iota(jnp.int32, (cells, relations, 3), 2) - 1
    cell = (target + step_x + shift[None, :, None] + 2 * cells) % cells
    match = cell[..., None] == jnp.arange(cells, dtype=jnp.int32)
    first = jnp.sum(jnp.where(match, blocks[None, :, 0, None, :], 0), -1)
    second = jnp.sum(jnp.where(match, blocks[None, :, 1, None, :], 0), -1)
    length = jnp.where(step_x == 0, first + second, jnp.where(step_x < 0, second, first))
    variant = jnp.where(step_x == 0, 0, 1)
    start = ((relation * cells + cell) * 2 + variant) * rooms + jnp.where(step_x < 0, first, 0)
    length = length.reshape(cells, -1)
    start = start.reshape(cells, -1)
    end = jnp.cumsum(length, axis=1)
    begin = end - length
    room = relations * 3 * rooms + 3 * PER_CHUNK
    room = (room + 127) // 128 * 128
    index = lax.broadcasted_iota(jnp.int32, (cells, relations * 3, room), 2)
    inside = (index >= begin[..., None]) & (index < end[..., None])
    zero_block = relations * cells * 2 * rooms
    block_list = zero_block + jnp.sum(
        jnp.where(inside, (start - begin)[..., None] + index - zero_block, 0), 1
    )
    chunks = (end[:, -1] + (PER_CHUNK - 1)) // PER_CHUNK

    own = padded[:3, 1, :, 1]
    targets = target_rows(tuple(4.0 * (own[k] - 0.5) for k in range(3)))

    smem = pl.BlockSpec(memory_space=pltpu.SMEM)
    vmem = pl.BlockSpec(memory_space=pltpu.VMEM)
    rows = PER_CHUNK * BLOCK
    density = pl.pallas_call(
        functools.partial(density_kernel, rooms),
        out_shape=jax.ShapeDtypeStruct((cells, slots), jnp.float32),
        in_specs=[smem, smem, smem, vmem, vmem, vmem],
        out_specs=vmem,
        scratch_shapes=[
            pltpu.VMEM((relations * cells * 2 * rooms + 1, BLOCK, 128), jnp.bfloat16),
            pltpu.VMEM((rows, 128), jnp.bfloat16),
            pltpu.VMEM((rows, 128), jnp.bfloat16),
            pltpu.VMEM((rows, slots + 128), jnp.float32),
            pltpu.VMEM((rows, slots + 128), jnp.float32),
        ],
        compiler_params=pltpu.CompilerParams(vmem_limit_bytes=56 * 1024 * 1024),
        name="density",
    )(block_list, chunks, counts.reshape(-1), pos, features, targets)
    return density.reshape(masses.shape)


def solution(mesh):
    in_specs = (
        P(None, "shear", None, "cross", None),
        P("shear", None, "cross", None),
        P("shear", None, "cross"),
        P(),
    )
    out_specs = P("shear", None, "cross", None)
    return jax.shard_map(shards, mesh=mesh, in_specs=in_specs, out_specs=out_specs, check_vma=False)
```

```python
import functools
import jax
import jax.numpy as jnp
from jax import lax
from jax.experimental import pallas as pl
from jax.experimental.pallas import tpu as pltpu
from jax.sharding import PartitionSpec as P

BLOCK = 16
PER_CHUNK = 8


def extended_2(block, sides, width):
    for axis, dim in sides:
        count = lax.axis_size(axis)
        forward = [(i, (i + 1) % count) for i in range(count)]
        backward = [(target, source) for source, target in forward]
        low = lax.ppermute(
            lax.slice_in_dim(block, block.shape[dim] - width, None, axis=dim), axis, forward
        )
        high = lax.ppermute(lax.slice_in_dim(block, 0, width, axis=dim), axis, backward)
        block = jnp.concatenate([low, block, high], axis=dim)
    return block


def parts(values):
    high = values.astype(jnp.bfloat16).astype(jnp.float32)
    rest = values - high
    middle = rest.astype(jnp.bfloat16).astype(jnp.float32)
    return high, middle, rest - middle


def source_rows(rows):
    high, middle, low = parts(rows)
    zero = jnp.zeros_like(rows)
    return [high, high, high, middle, middle, low, zero, zero]


def target_rows(rows):
    high, middle, low = parts(rows)
    zero = jnp.zeros_like(rows)
    return [high, middle, low, high, middle, high, zero, zero]


def density_kernel(
    rooms, list_ref, chunks_ref, counts_ref, pos_ref, data_ref, out_ref,
    store_ref, mask_ref, sq_a, sq_b,
):
    cells, slots = out_ref.shape
    pairs = pos_ref.shape[0]
    unroll = 4
    zero_block = pairs * rooms
    store_ref[zero_block] = jnp.zeros((BLOCK, 128), jnp.bfloat16)
    lane = lax.broadcasted_iota(jnp.int32, (BLOCK, 128), 1)
    mask_ref[0] = jnp.where(lane < 64, 1.0, 0.0).astype(jnp.bfloat16)
    mask_ref[1] = jnp.where(lane < 64, 0.0, 1.0).astype(jnp.bfloat16)
    row_id = lax.broadcasted_iota(jnp.int32, (rooms * BLOCK, slots), 0)
    row = lax.broadcasted_iota(jnp.int32, (8, slots), 0)

    def assembled(scaled, raw):
        squares = jnp.where(row < 3, scaled * scaled, 0.0)
        norm = jnp.sum(squares, axis=0, keepdims=True)
        rows = jnp.where(row < 3, scaled, raw)
        rows = jnp.where(row == 4, norm, rows)
        return jnp.where(row == 5, 1.0, jnp.where(row > 5, 0.0, rows))

    def compact(step, carry):
        for k in range(unroll):
            pair = step * unroll + k
            relation = pair // cells
            step_y = (relation // 3 - 1).astype(jnp.float32)
            step_z = (relation % 3 - 1).astype(jnp.float32)
            raw = data_ref[pair]
            raw = jnp.concatenate([raw, raw], axis=0)
            offset = jnp.where(row == 0, step_y, jnp.where(row == 2, step_z, 0.0)) - 0.5
            scaled = 4.0 * (raw + offset)
            moved = scaled + jnp.where(row == 1, jnp.where(raw <= 0.5, 4.0, -4.0), 0.0)
            features = jnp.concatenate(
                source_rows(assembled(scaled, raw)) + source_rows(assembled(moved, raw)), axis=0
            ).astype(jnp.bfloat16)
            chosen = jnp.where(row_id == pos_ref[pair], 1.0, 0.0).astype(jnp.bfloat16)
            rows = lax.dot_general(
                chosen, features, (((1,), (1,)), ((), ())), preferred_element_type=jnp.float32
            )
            store_ref[pl.ds(pair * rooms, rooms)] = rows.astype(jnp.bfloat16).reshape(
                rooms, BLOCK, 128
            )
        return carry

    lax.fori_loop(0, pairs // unroll, compact, 0)
    own = (pairs // cells) // 2 * cells
    spread = jnp.where(lax.broadcasted_iota(jnp.int32, (8, 128), 0) == 3, 1.0, 0.0)

    def cell_body(cell, carry):
        raw = data_ref[own + cell]
        raw = jnp.concatenate([raw, raw], axis=0)
        scaled = 4.0 * (raw - 0.5)
        norm = jnp.sum(jnp.where(row < 3, scaled * scaled, 0.0), axis=0, keepdims=True)
        rows = jnp.where(row < 3, -2.0 * scaled, 0.0)
        rows = jnp.where(row == 4, 1.0, jnp.where(row == 5, norm, rows))
        half = target_rows(jnp.concatenate([rows, spread], axis=1))
        weights = jnp.concatenate(half + half, axis=0).astype(jnp.bfloat16)

        def produce(chunk, sq_ref):
            blocks = []
            for k in range(PER_CHUNK):
                entry = list_ref[cell, chunk * PER_CHUNK + k]
                blocks.append(store_ref[entry >> 1] * mask_ref[entry & 1])
            lhs = jnp.concatenate(blocks, axis=0)
            sq_ref[...] = jnp.dot(lhs, weights, preferred_element_type=jnp.float32)

        def consume(sq_ref, acc):
            for group in range(PER_CHUNK * BLOCK // 8):
                rows = pl.ds(group * 8, 8)
                mass = sq_ref[rows, slots:]
                sums = []
                for tile in range(slots // 128):
                    lanes = slice(tile * 128, tile * 128 + 128)
                    squared = jnp.maximum(sq_ref[rows, lanes], 1e-30)
                    q = squared * lax.rsqrt(squared)
                    outer = jnp.maximum(2.0 - q, 0.0)
                    inner = jnp.maximum(outer - 1.0, 0.0)
                    value = outer * outer * outer - 4.0 * (inner * inner * inner)
                    sums.append(acc[tile] + mass * value)
                acc = tuple(sums)
            return acc

        produce(0, sq_a)

        def pair_body(step, acc):
            produce(2 * step + 1, sq_b)
            acc = consume(sq_a, acc)
            produce(2 * step + 2, sq_a)
            return consume(sq_b, acc)

        empty = tuple(jnp.zeros((8, 128), jnp.float32) for _ in range(slots // 128))
        acc = lax.fori_loop(0, (chunks_ref[cell] + 1) // 2, pair_body, empty)
        total = jnp.sum(jnp.concatenate(acc, axis=1), axis=0, keepdims=True)
        total = total * (16.0 / 3.141592653589793)
        slot = lax.broadcasted_iota(jnp.int32, (1, slots), 1)
        out_ref[pl.ds(cell, 1), :] = jnp.where(slot < counts_ref[cell], total, 0.0)
        return carry

    lax.fori_loop(0, cells, cell_body, 0)


def shards(positions, masses, counts, shear_offset):
    cells_y, cells, cells_z, slots = masses.shape
    assert cells_y == 1 and cells_z == 1
    rooms = slots // BLOCK + 1
    slot_index = lax.broadcasted_iota(jnp.int32, masses.shape, 3)
    weight = jnp.where(slot_index < counts[..., None], masses, jnp.float32(0.0))
    data = jnp.stack(
        [positions[0, 0, :, 0], positions[1, 0, :, 0], positions[2, 0, :, 0], weight[0, :, 0]], 1
    )[None, None]
    offset = shear_offset[0]
    shear_index = lax.axis_index("shear")
    cycle = lax.axis_size("shear")
    padded = extended_2(data, (("shear", 0), ("cross", 1)), 1)
    low_shift = jnp.where(shear_index == 0, -offset, 0)
    high_shift = jnp.where(shear_index == cycle - 1, offset, 0)

    masks, shifts = [], []
    for step_y in (-1, 0, 1):
        for step_z in (-1, 0, 1):
            y, x, z, mass = (padded[1 + step_y, 1 + step_z, :, k] for k in range(4))
            keep = mass > 0.0
            for value, step in ((y, step_y), (z, step_z)):
                if step == -1:
                    keep = keep & (value >= 0.5)
                elif step == 1:
                    keep = keep & (value <= 0.5)
            lower = x <= 0.5
            masks.append(jnp.stack([keep & lower, keep & ~lower], 0))
            shifts.append({-1: low_shift, 0: jnp.int32(0), 1: high_shift}[step_y])
    chosen = jnp.stack(masks, 0)
    triangle = (
        lax.broadcasted_iota(jnp.int32, (slots, slots), 0)
        <= lax.broadcasted_iota(jnp.int32, (slots, slots), 1)
    ).astype(jnp.bfloat16)
    ranks = jnp.dot(
        chosen.reshape(-1, slots).astype(jnp.bfloat16), triangle,
        preferred_element_type=jnp.float32,
    ).astype(jnp.int32).reshape(chosen.shape)
    sizes = ranks[..., -1]
    blocks = (sizes + (BLOCK - 1)) // BLOCK
    pos = jnp.where(
        chosen[:, 0],
        ranks[:, 0] - 1,
        jnp.where(chosen[:, 1], ranks[:, 1] - 1 + BLOCK * blocks[:, 0, :, None], -1),
    ).reshape(-1, 1, slots)

    relations = len(masks)
    shift = jnp.stack(shifts)
    target = lax.broadcasted_iota(jnp.int32, (cells, relations, 3), 0)
    relation = lax.broadcasted_iota(jnp.int32, (cells, relations, 3), 1)
    step_x = lax.broadcasted_iota(jnp.int32, (cells, relations, 3), 2) - 1
    cell = (target + step_x + shift[None, :, None] + 2 * cells) % cells
    match = cell[..., None] == jnp.arange(cells, dtype=jnp.int32)
    first = jnp.sum(jnp.where(match, blocks[None, :, 0, None, :], 0), -1)
    second = jnp.sum(jnp.where(match, blocks[None, :, 1, None, :], 0), -1)
    length = jnp.where(step_x == 0, first + second, jnp.where(step_x < 0, second, first))
    variant = jnp.where(step_x == 0, 0, 1)
    start = (relation * cells + cell) * rooms + jnp.where(step_x < 0, first, 0)
    start = 2 * start + variant
    length = length.reshape(cells, -1)
    start = start.reshape(cells, -1)
    end = jnp.cumsum(length, axis=1)
    begin = end - length
    room = relations * 3 * rooms + 3 * PER_CHUNK
    room = (room + 127) // 128 * 128
    index = lax.broadcasted_iota(jnp.int32, (cells, relations * 3, room), 2)
    inside = (index >= begin[..., None]) & (index < end[..., None])
    zero_block = 2 * relations * cells * rooms
    block_list = zero_block + jnp.sum(
        jnp.where(inside, (start - 2 * begin)[..., None] + 2 * index - zero_block, 0), 1
    )
    chunks = (end[:, -1] + (PER_CHUNK - 1)) // PER_CHUNK

    smem = pl.BlockSpec(memory_space=pltpu.SMEM)
    vmem = pl.BlockSpec(memory_space=pltpu.VMEM)
    rows = PER_CHUNK * BLOCK
    density = pl.pallas_call(
        functools.partial(density_kernel, rooms),
        out_shape=jax.ShapeDtypeStruct((cells, slots), jnp.float32),
        in_specs=[smem, smem, smem, vmem, vmem],
        out_specs=vmem,
        scratch_shapes=[
            pltpu.VMEM((relations * cells * rooms + 1, BLOCK, 128), jnp.bfloat16),
            pltpu.VMEM((2, BLOCK, 128), jnp.bfloat16),
            pltpu.VMEM((rows, slots + 128), jnp.float32),
            pltpu.VMEM((rows, slots + 128), jnp.float32),
        ],
        compiler_params=pltpu.CompilerParams(vmem_limit_bytes=56 * 1024 * 1024),
        name="density",
    )(block_list, chunks, counts.reshape(-1), pos, padded.reshape(-1, 4, slots))
    return density.reshape(masses.shape)


def solution(mesh):
    in_specs = (
        P(None, "shear", None, "cross", None),
        P("shear", None, "cross", None),
        P("shear", None, "cross"),
        P(),
    )
    out_specs = P("shear", None, "cross", None)
    return jax.shard_map(shards, mesh=mesh, in_specs=in_specs, out_specs=out_specs, check_vma=False)
```

```python
import functools
import jax
import jax.numpy as jnp
from jax import lax
from jax.experimental import pallas as pl
from jax.experimental.pallas import tpu as pltpu
from jax.sharding import PartitionSpec as P

BLOCK = 16
PER_CHUNK = 8


def halo_kernel(data_ref, out_ref, send_sems, recv_sems, local_sem):
    shear, cross = lax.axis_index("shear"), lax.axis_index("cross")
    rows, planes = lax.axis_size("shear"), lax.axis_size("cross")
    mesh_ids = pl.DeviceIdType.MESH
    along_y = [(lax.rem(shear + rows - step, rows), cross) for step in (-1, 1)]
    along_z = [(shear, lax.rem(cross + planes - step, planes)) for step in (-1, 1)]
    barrier = pltpu.get_barrier_semaphore()
    for device in along_y + along_z:
        pl.semaphore_signal(barrier, inc=1, device_id=device, device_id_type=mesh_ids)
    own = pltpu.make_async_copy(data_ref, out_ref.at[1, 1], local_sem)
    own.start()
    pl.semaphore_wait(barrier, 4)

    def sent(source, y, z, device):
        slot = 3 * y + z
        copy = pltpu.make_async_remote_copy(
            src_ref=source,
            dst_ref=out_ref.at[y, z],
            send_sem=send_sems.at[slot],
            recv_sem=recv_sems.at[slot],
            device_id=device,
            device_id_type=mesh_ids,
        )
        copy.start()
        return copy

    rows_sent = [sent(data_ref, y, 1, along_y[k]) for k, y in enumerate((0, 2))]
    planes_sent = [sent(data_ref, 1, z, along_z[k]) for k, z in enumerate((0, 2))]
    for k, y in enumerate((0, 2)):
        rows_sent[k].wait_recv()
        for j, z in enumerate((0, 2)):
            planes_sent.append(sent(out_ref.at[y, 1], y, z, along_z[j]))
    for copy in rows_sent:
        copy.wait_send()
    for copy in planes_sent:
        copy.wait()
    own.wait()


def halo(data):
    vmem = pl.BlockSpec(memory_space=pltpu.VMEM)
    return pl.pallas_call(
        halo_kernel,
        out_shape=jax.ShapeDtypeStruct((3, 3) + data.shape, data.dtype),
        in_specs=[vmem],
        out_specs=vmem,
        scratch_shapes=[
            pltpu.SemaphoreType.DMA((9,)),
            pltpu.SemaphoreType.DMA((9,)),
            pltpu.SemaphoreType.DMA,
        ],
        compiler_params=pltpu.CompilerParams(collective_id=0, has_side_effects=True),
        name="halo",
    )(data)


def parts(values):
    high = values.astype(jnp.bfloat16).astype(jnp.float32)
    rest = values - high
    middle = rest.astype(jnp.bfloat16).astype(jnp.float32)
    return high, middle, rest - middle


def source_rows(rows):
    high, middle, low = parts(rows)
    zero = jnp.zeros_like(rows)
    return [high, high, high, middle, middle, low, zero, zero]


def target_rows(rows):
    high, middle, low = parts(rows)
    zero = jnp.zeros_like(rows)
    return [high, middle, low, high, middle, high, zero, zero]


def density_kernel(
    rooms, list_ref, chunks_ref, counts_ref, used_ref, pos_ref, data_ref, out_ref,
    store_ref, mask_ref, sq_a, sq_b,
):
    cells, slots = out_ref.shape
    pairs = pos_ref.shape[0]
    unroll = 4
    zero_block = pairs * rooms
    store_ref[zero_block] = jnp.zeros((BLOCK, 128), jnp.bfloat16)
    lane = lax.broadcasted_iota(jnp.int32, (BLOCK, 128), 1)
    mask_ref[0] = jnp.where(lane < 64, 1.0, 0.0).astype(jnp.bfloat16)
    mask_ref[1] = jnp.where(lane < 64, 0.0, 1.0).astype(jnp.bfloat16)
    row_id = lax.broadcasted_iota(jnp.int32, (rooms * BLOCK, slots), 0)
    row = lax.broadcasted_iota(jnp.int32, (8, slots), 0)

    def assembled(scaled, raw):
        squares = jnp.where(row < 3, scaled * scaled, 0.0)
        norm = jnp.sum(squares, axis=0, keepdims=True)
        rows = jnp.where(row < 3, scaled, raw)
        rows = jnp.where(row == 4, norm, rows)
        return jnp.where(row == 5, 1.0, jnp.where(row > 5, 0.0, rows))

    first_rooms = rooms // 2 + 2

    def fill(batch, begin, count):
        for pair, features in batch:
            chosen = jnp.where(
                row_id[: count * BLOCK] == pos_ref[pair] - begin * BLOCK, 1.0, 0.0
            ).astype(jnp.bfloat16)
            rows = lax.dot_general(
                chosen, features, (((1,), (1,)), ((), ())), preferred_element_type=jnp.float32
            )
            store_ref[pl.ds(pair * rooms + begin, count)] = rows.astype(jnp.bfloat16).reshape(
                count, BLOCK, 128
            )

    def compact(step, carry):
        batch = []
        for k in range(unroll):
            pair = step * unroll + k
            relation = pair // cells
            step_y = (relation // 3 - 1).astype(jnp.float32)
            step_z = (relation % 3 - 1).astype(jnp.float32)
            raw = data_ref[pair]
            raw = jnp.concatenate([raw, raw], axis=0)
            offset = jnp.where(row == 0, step_y, jnp.where(row == 2, step_z, 0.0)) - 0.5
            scaled = 4.0 * (raw + offset)
            moved = scaled + jnp.where(row == 1, jnp.where(raw <= 0.5, 4.0, -4.0), 0.0)
            features = jnp.concatenate(
                source_rows(assembled(scaled, raw)) + source_rows(assembled(moved, raw)), axis=0
            ).astype(jnp.bfloat16)
            batch.append((pair, features))
        fill(batch, 0, first_rooms)
        most = used_ref[step * unroll]
        for k in range(1, unroll):
            most = jnp.maximum(most, used_ref[step * unroll + k])

        @pl.when(most > first_rooms)
        def _():
            fill(batch, first_rooms, rooms - first_rooms)

        return carry

    lax.fori_loop(0, pairs // unroll, compact, 0)
    own = (pairs // cells) // 2 * cells
    spread = jnp.where(lax.broadcasted_iota(jnp.int32, (8, 128), 0) == 3, 1.0, 0.0)

    def cell_body(cell, carry):
        raw = data_ref[own + cell]
        raw = jnp.concatenate([raw, raw], axis=0)
        scaled = 4.0 * (raw - 0.5)
        norm = jnp.sum(jnp.where(row < 3, scaled * scaled, 0.0), axis=0, keepdims=True)
        rows = jnp.where(row < 3, -2.0 * scaled, 0.0)
        rows = jnp.where(row == 4, 1.0, jnp.where(row == 5, norm, rows))
        half = target_rows(jnp.concatenate([rows, spread], axis=1))
        weights = jnp.concatenate(half + half, axis=0).astype(jnp.bfloat16)

        def produce(chunk, sq_ref):
            blocks = []
            for k in range(PER_CHUNK):
                entry = list_ref[cell, chunk * PER_CHUNK + k]
                blocks.append(store_ref[entry >> 1] * mask_ref[entry & 1])
            lhs = jnp.concatenate(blocks, axis=0)
            sq_ref[...] = jnp.dot(lhs, weights, preferred_element_type=jnp.float32)

        def consume(sq_ref, acc):
            for group in range(PER_CHUNK * BLOCK // 8):
                rows = pl.ds(group * 8, 8)
                mass = sq_ref[rows, slots:]
                sums = []
                for tile in range(slots // 128):
                    lanes = slice(tile * 128, tile * 128 + 128)
                    squared = jnp.maximum(sq_ref[rows, lanes], 1e-30)
                    q = squared * lax.rsqrt(squared)
                    outer = jnp.maximum(2.0 - q, 0.0)
                    inner = jnp.maximum(outer - 1.0, 0.0)
                    value = outer * outer * outer - 4.0 * (inner * inner * inner)
                    sums.append(acc[tile] + mass * value)
                acc = tuple(sums)
            return acc

        produce(0, sq_a)

        def pair_body(step, acc):
            produce(2 * step + 1, sq_b)
            acc = consume(sq_a, acc)
            produce(2 * step + 2, sq_a)
            return consume(sq_b, acc)

        empty = tuple(jnp.zeros((8, 128), jnp.float32) for _ in range(slots // 128))
        acc = lax.fori_loop(0, (chunks_ref[cell] + 1) // 2, pair_body, empty)
        total = jnp.sum(jnp.concatenate(acc, axis=1), axis=0, keepdims=True)
        total = total * (16.0 / 3.141592653589793)
        slot = lax.broadcasted_iota(jnp.int32, (1, slots), 1)
        out_ref[pl.ds(cell, 1), :] = jnp.where(slot < counts_ref[cell], total, 0.0)
        return carry

    lax.fori_loop(0, cells, cell_body, 0)


def shards(positions, masses, counts, shear_offset):
    cells_y, cells, cells_z, slots = masses.shape
    assert cells_y == 1 and cells_z == 1
    rooms = slots // BLOCK + 1
    slot_index = lax.broadcasted_iota(jnp.int32, masses.shape, 3)
    weight = jnp.where(slot_index < counts[..., None], masses, jnp.float32(0.0))
    data = jnp.stack(
        [positions[0, 0, :, 0], positions[1, 0, :, 0], positions[2, 0, :, 0], weight[0, :, 0]], 1
    )
    offset = shear_offset[0]
    shear_index = lax.axis_index("shear")
    cycle = lax.axis_size("shear")
    padded = halo(data)
    low_shift = jnp.where(shear_index == 0, -offset, 0)
    high_shift = jnp.where(shear_index == cycle - 1, offset, 0)

    masks, shifts = [], []
    for step_y in (-1, 0, 1):
        for step_z in (-1, 0, 1):
            y, x, z, mass = (padded[1 + step_y, 1 + step_z, :, k] for k in range(4))
            keep = mass > 0.0
            for value, step in ((y, step_y), (z, step_z)):
                if step == -1:
                    keep = keep & (value >= 0.5)
                elif step == 1:
                    keep = keep & (value <= 0.5)
            lower = x <= 0.5
            masks.append(jnp.stack([keep & lower, keep & ~lower], 0))
            shifts.append({-1: low_shift, 0: jnp.int32(0), 1: high_shift}[step_y])
    chosen = jnp.stack(masks, 0)
    triangle = (
        lax.broadcasted_iota(jnp.int32, (slots, slots), 0)
        <= lax.broadcasted_iota(jnp.int32, (slots, slots), 1)
    ).astype(jnp.bfloat16)
    ranks = jnp.dot(
        chosen.reshape(-1, slots).astype(jnp.bfloat16), triangle,
        preferred_element_type=jnp.float32,
    ).astype(jnp.int32).reshape(chosen.shape)
    sizes = ranks[..., -1]
    blocks = (sizes + (BLOCK - 1)) // BLOCK
    pos = jnp.where(
        chosen[:, 0],
        ranks[:, 0] - 1,
        jnp.where(chosen[:, 1], ranks[:, 1] - 1 + BLOCK * blocks[:, 0, :, None], -1),
    ).reshape(-1, 1, slots)

    relations = len(masks)
    shift = jnp.stack(shifts)
    target = lax.broadcasted_iota(jnp.int32, (cells, relations, 3), 0)
    relation = lax.broadcasted_iota(jnp.int32, (cells, relations, 3), 1)
    step_x = lax.broadcasted_iota(jnp.int32, (cells, relations, 3), 2) - 1
    cell = (target + step_x + shift[None, :, None] + 2 * cells) % cells
    match = cell[..., None] == jnp.arange(cells, dtype=jnp.int32)
    first = jnp.sum(jnp.where(match, blocks[None, :, 0, None, :], 0), -1)
    second = jnp.sum(jnp.where(match, blocks[None, :, 1, None, :], 0), -1)
    length = jnp.where(step_x == 0, first + second, jnp.where(step_x < 0, second, first))
    variant = jnp.where(step_x == 0, 0, 1)
    start = (relation * cells + cell) * rooms + jnp.where(step_x < 0, first, 0)
    start = 2 * start + variant
    length = length.reshape(cells, -1)
    start = start.reshape(cells, -1)
    end = jnp.cumsum(length, axis=1)
    begin = end - length
    room = relations * 3 * rooms + 3 * PER_CHUNK
    room = (room + 127) // 128 * 128
    index = lax.broadcasted_iota(jnp.int32, (cells, relations * 3, room), 2)
    inside = (index >= begin[..., None]) & (index < end[..., None])
    zero_block = 2 * relations * cells * rooms
    block_list = zero_block + jnp.sum(
        jnp.where(inside, (start - 2 * begin)[..., None] + 2 * index - zero_block, 0), 1
    )
    chunks = (end[:, -1] + (PER_CHUNK - 1)) // PER_CHUNK

    smem = pl.BlockSpec(memory_space=pltpu.SMEM)
    vmem = pl.BlockSpec(memory_space=pltpu.VMEM)
    rows = PER_CHUNK * BLOCK
    density = pl.pallas_call(
        functools.partial(density_kernel, rooms),
        out_shape=jax.ShapeDtypeStruct((cells, slots), jnp.float32),
        in_specs=[smem, smem, smem, smem, vmem, vmem],
        out_specs=vmem,
        scratch_shapes=[
            pltpu.VMEM((relations * cells * rooms + 1, BLOCK, 128), jnp.bfloat16),
            pltpu.VMEM((2, BLOCK, 128), jnp.bfloat16),
            pltpu.VMEM((rows, slots + 128), jnp.float32),
            pltpu.VMEM((rows, slots + 128), jnp.float32),
        ],
        compiler_params=pltpu.CompilerParams(vmem_limit_bytes=56 * 1024 * 1024),
        name="density",
    )(block_list, chunks, counts.reshape(-1), jnp.sum(blocks, 1).reshape(-1), pos, padded.reshape(-1, 4, slots))
    return density.reshape(masses.shape)


def solution(mesh):
    in_specs = (
        P(None, "shear", None, "cross", None),
        P("shear", None, "cross", None),
        P("shear", None, "cross"),
        P(),
    )
    out_specs = P("shear", None, "cross", None)
    return jax.shard_map(shards, mesh=mesh, in_specs=in_specs, out_specs=out_specs, check_vma=False)
```

```python
import functools
import jax
import jax.numpy as jnp
from jax import lax
from jax.experimental import pallas as pl
from jax.experimental.pallas import tpu as pltpu
from jax.sharding import PartitionSpec as P

BLOCK = 16
PER_CHUNK = 8


def halo_kernel(data_ref, out_ref, send_sems, recv_sems, local_sem):
    shear, cross = lax.axis_index("shear"), lax.axis_index("cross")
    rows, planes = lax.axis_size("shear"), lax.axis_size("cross")
    mesh_ids = pl.DeviceIdType.MESH
    along_y = [(lax.rem(shear + rows - step, rows), cross) for step in (-1, 1)]
    along_z = [(shear, lax.rem(cross + planes - step, planes)) for step in (-1, 1)]
    barrier = pltpu.get_barrier_semaphore()
    for device in along_y + along_z:
        pl.semaphore_signal(barrier, inc=1, device_id=device, device_id_type=mesh_ids)
    own = pltpu.make_async_copy(data_ref, out_ref.at[1, 1], local_sem)
    own.start()
    pl.semaphore_wait(barrier, 4)

    def sent(source, y, z, device):
        slot = 3 * y + z
        copy = pltpu.make_async_remote_copy(
            src_ref=source,
            dst_ref=out_ref.at[y, z],
            send_sem=send_sems.at[slot],
            recv_sem=recv_sems.at[slot],
            device_id=device,
            device_id_type=mesh_ids,
        )
        copy.start()
        return copy

    rows_sent = [sent(data_ref, y, 1, along_y[k]) for k, y in enumerate((0, 2))]
    planes_sent = [sent(data_ref, 1, z, along_z[k]) for k, z in enumerate((0, 2))]
    for k, y in enumerate((0, 2)):
        rows_sent[k].wait_recv()
        for j, z in enumerate((0, 2)):
            planes_sent.append(sent(out_ref.at[y, 1], y, z, along_z[j]))
    for copy in rows_sent:
        copy.wait_send()
    for copy in planes_sent:
        copy.wait()
    own.wait()


def halo(data):
    vmem = pl.BlockSpec(memory_space=pltpu.VMEM)
    return pl.pallas_call(
        halo_kernel,
        out_shape=jax.ShapeDtypeStruct((3, 3) + data.shape, data.dtype),
        in_specs=[vmem],
        out_specs=vmem,
        scratch_shapes=[
            pltpu.SemaphoreType.DMA((9,)),
            pltpu.SemaphoreType.DMA((9,)),
            pltpu.SemaphoreType.DMA,
        ],
        compiler_params=pltpu.CompilerParams(collective_id=0, has_side_effects=True),
        name="halo",
    )(data)


def parts(values):
    high = values.astype(jnp.bfloat16).astype(jnp.float32)
    rest = values - high
    middle = rest.astype(jnp.bfloat16).astype(jnp.float32)
    return high, middle, rest - middle


def source_rows(rows):
    high, middle, low = parts(rows)
    zero = jnp.zeros_like(rows)
    return [high, high, high, middle, middle, low, zero, zero]


def target_rows(rows):
    high, middle, low = parts(rows)
    zero = jnp.zeros_like(rows)
    return [high, middle, low, high, middle, high, zero, zero]


def density_kernel(
    rooms, list_ref, chunks_ref, counts_ref, used_ref, pos_ref, data_ref, out_ref,
    store_ref, mask_ref, sq_a, sq_b,
):
    cells, slots = out_ref.shape
    pairs = pos_ref.shape[0]
    unroll = 4
    zero_block = pairs * rooms
    store_ref[zero_block] = jnp.zeros((BLOCK, 128), jnp.bfloat16)
    lane = lax.broadcasted_iota(jnp.int32, (BLOCK, 128), 1)
    mask_ref[0] = jnp.where(lane < 64, 1.0, 0.0).astype(jnp.bfloat16)
    mask_ref[1] = jnp.where(lane < 64, 0.0, 1.0).astype(jnp.bfloat16)
    row_id = lax.broadcasted_iota(jnp.int32, (rooms * BLOCK, slots), 0)
    row = lax.broadcasted_iota(jnp.int32, (8, slots), 0)

    def assembled(scaled, raw):
        squares = jnp.where(row < 3, scaled * scaled, 0.0)
        norm = jnp.sum(squares, axis=0, keepdims=True)
        rows = jnp.where(row < 3, scaled, raw)
        rows = jnp.where(row == 4, norm, rows)
        return jnp.where(row == 5, 1.0, jnp.where(row > 5, 0.0, rows))

    first_rooms = rooms // 2 + 2

    def fill(batch, begin, count):
        for pair, features in batch:
            chosen = jnp.where(
                row_id[: count * BLOCK] == pos_ref[pair] - begin * BLOCK, 1.0, 0.0
            ).astype(jnp.bfloat16)
            rows = lax.dot_general(
                chosen, features, (((1,), (1,)), ((), ())), preferred_element_type=jnp.float32
            )
            store_ref[pl.ds(pair * rooms + begin, count)] = rows.astype(jnp.bfloat16).reshape(
                count, BLOCK, 128
            )

    def compact(step, carry):
        batch = []
        for k in range(unroll):
            pair = step * unroll + k
            relation = pair // cells
            step_y = (relation // 3 - 1).astype(jnp.float32)
            step_z = (relation % 3 - 1).astype(jnp.float32)
            raw = data_ref[pair]
            raw = jnp.concatenate([raw, raw], axis=0)
            offset = jnp.where(row == 0, step_y, jnp.where(row == 2, step_z, 0.0)) - 0.5
            scaled = 4.0 * (raw + offset)
            moved = scaled + jnp.where(row == 1, jnp.where(raw <= 0.5, 4.0, -4.0), 0.0)
            features = jnp.concatenate(
                source_rows(assembled(scaled, raw)) + source_rows(assembled(moved, raw)), axis=0
            ).astype(jnp.bfloat16)
            batch.append((pair, features))
        fill(batch, 0, first_rooms)
        most = used_ref[step * unroll]
        for k in range(1, unroll):
            most = jnp.maximum(most, used_ref[step * unroll + k])

        @pl.when(most > first_rooms)
        def _():
            fill(batch, first_rooms, rooms - first_rooms)

        return carry

    lax.fori_loop(0, pairs // unroll, compact, 0)
    own = (pairs // cells) // 2 * cells
    spread = jnp.where(lax.broadcasted_iota(jnp.int32, (8, 128), 0) == 3, 1.0, 0.0)

    def cell_body(cell, width):
        raw = data_ref[own + cell]
        raw = jnp.concatenate([raw, raw], axis=0)
        scaled = 4.0 * (raw - 0.5)
        norm = jnp.sum(jnp.where(row < 3, scaled * scaled, 0.0), axis=0, keepdims=True)
        rows = jnp.where(row < 3, -2.0 * scaled, 0.0)
        rows = jnp.where(row == 4, 1.0, jnp.where(row == 5, norm, rows))
        half = target_rows(jnp.concatenate([rows[:, :width], spread], axis=1))
        weights = jnp.concatenate(half + half, axis=0).astype(jnp.bfloat16)

        def produce(chunk, sq_ref):
            blocks = []
            for k in range(PER_CHUNK):
                entry = list_ref[cell, chunk * PER_CHUNK + k]
                blocks.append(store_ref[entry >> 1] * mask_ref[entry & 1])
            lhs = jnp.concatenate(blocks, axis=0)
            sq_ref[:, : width + 128] = jnp.dot(lhs, weights, preferred_element_type=jnp.float32)

        def consume(sq_ref, acc):
            for group in range(PER_CHUNK * BLOCK // 8):
                rows = pl.ds(group * 8, 8)
                mass = sq_ref[rows, width : width + 128]
                sums = []
                for tile in range(width // 128):
                    lanes = slice(tile * 128, tile * 128 + 128)
                    squared = jnp.maximum(sq_ref[rows, lanes], 1e-30)
                    q = squared * lax.rsqrt(squared)
                    outer = jnp.maximum(2.0 - q, 0.0)
                    inner = jnp.maximum(outer - 1.0, 0.0)
                    value = outer * outer * outer - 4.0 * (inner * inner * inner)
                    sums.append(acc[tile] + mass * value)
                acc = tuple(sums)
            return acc

        produce(0, sq_a)

        def pair_body(step, acc):
            produce(2 * step + 1, sq_b)
            acc = consume(sq_a, acc)
            produce(2 * step + 2, sq_a)
            return consume(sq_b, acc)

        empty = tuple(jnp.zeros((8, 128), jnp.float32) for _ in range(width // 128))
        acc = lax.fori_loop(0, (chunks_ref[cell] + 1) // 2, pair_body, empty)
        total = jnp.sum(jnp.concatenate(acc, axis=1), axis=0, keepdims=True)
        total = total * (16.0 / 3.141592653589793)
        if width < slots:
            total = jnp.concatenate([total, jnp.zeros((1, slots - width), jnp.float32)], axis=1)
        slot = lax.broadcasted_iota(jnp.int32, (1, slots), 1)
        out_ref[pl.ds(cell, 1), :] = jnp.where(slot < counts_ref[cell], total, 0.0)

    def sized_body(cell, carry):
        @pl.when(counts_ref[cell] <= 128)
        def _():
            cell_body(cell, 128)

        @pl.when(counts_ref[cell] > 128)
        def _():
            cell_body(cell, slots)

        return carry

    lax.fori_loop(0, cells, sized_body, 0)


def shards(positions, masses, counts, shear_offset):
    cells_y, cells, cells_z, slots = masses.shape
    assert cells_y == 1 and cells_z == 1
    rooms = slots // BLOCK + 1
    slot_index = lax.broadcasted_iota(jnp.int32, masses.shape, 3)
    weight = jnp.where(slot_index < counts[..., None], masses, jnp.float32(0.0))
    data = jnp.stack(
        [positions[0, 0, :, 0], positions[1, 0, :, 0], positions[2, 0, :, 0], weight[0, :, 0]], 1
    )
    offset = shear_offset[0]
    shear_index = lax.axis_index("shear")
    cycle = lax.axis_size("shear")
    padded = halo(data)
    low_shift = jnp.where(shear_index == 0, -offset, 0)
    high_shift = jnp.where(shear_index == cycle - 1, offset, 0)

    relations = 9
    values = padded.reshape(relations, cells, 4, slots)
    y, x, z, mass = (values[:, :, k] for k in range(4))
    which = lax.broadcasted_iota(jnp.int32, y.shape, 0)
    keep = mass > 0.0
    for value, step in ((y, which // 3 - 1), (z, which % 3 - 1)):
        keep = keep & ((step != -1) | (value >= 0.5)) & ((step != 1) | (value <= 0.5))
    lower = x <= 0.5
    chosen = jnp.stack([keep & lower, keep & ~lower], 1)
    shifts = [low_shift] * 3 + [jnp.int32(0)] * 3 + [high_shift] * 3
    triangle = (
        lax.broadcasted_iota(jnp.int32, (slots, slots), 0)
        <= lax.broadcasted_iota(jnp.int32, (slots, slots), 1)
    ).astype(jnp.bfloat16)
    ranks = jnp.dot(
        chosen.reshape(-1, slots).astype(jnp.bfloat16), triangle,
        preferred_element_type=jnp.float32,
    ).astype(jnp.int32).reshape(chosen.shape)
    sizes = ranks[..., -1]
    blocks = (sizes + (BLOCK - 1)) // BLOCK
    pos = jnp.where(
        chosen[:, 0],
        ranks[:, 0] - 1,
        jnp.where(chosen[:, 1], ranks[:, 1] - 1 + BLOCK * blocks[:, 0, :, None], -1),
    ).reshape(-1, 1, slots)

    shift = jnp.stack(shifts)
    target = lax.broadcasted_iota(jnp.int32, (cells, relations, 3), 0)
    relation = lax.broadcasted_iota(jnp.int32, (cells, relations, 3), 1)
    step_x = lax.broadcasted_iota(jnp.int32, (cells, relations, 3), 2) - 1
    cell = (target + step_x + shift[None, :, None] + 2 * cells) % cells
    match = cell[..., None] == jnp.arange(cells, dtype=jnp.int32)
    first = jnp.sum(jnp.where(match, blocks[None, :, 0, None, :], 0), -1)
    second = jnp.sum(jnp.where(match, blocks[None, :, 1, None, :], 0), -1)
    length = jnp.where(step_x == 0, first + second, jnp.where(step_x < 0, second, first))
    variant = jnp.where(step_x == 0, 0, 1)
    start = (relation * cells + cell) * rooms + jnp.where(step_x < 0, first, 0)
    start = 2 * start + variant
    length = length.reshape(cells, -1)
    start = start.reshape(cells, -1)
    end = jnp.cumsum(length, axis=1)
    begin = end - length
    room = relations * 3 * rooms + 3 * PER_CHUNK
    room = (room + 127) // 128 * 128
    index = lax.broadcasted_iota(jnp.int32, (cells, relations * 3, room), 2)
    inside = (index >= begin[..., None]) & (index < end[..., None])
    zero_block = 2 * relations * cells * rooms
    block_list = zero_block + jnp.sum(
        jnp.where(inside, (start - 2 * begin)[..., None] + 2 * index - zero_block, 0), 1
    )
    chunks = (end[:, -1] + (PER_CHUNK - 1)) // PER_CHUNK

    smem = pl.BlockSpec(memory_space=pltpu.SMEM)
    vmem = pl.BlockSpec(memory_space=pltpu.VMEM)
    rows = PER_CHUNK * BLOCK
    density = pl.pallas_call(
        functools.partial(density_kernel, rooms),
        out_shape=jax.ShapeDtypeStruct((cells, slots), jnp.float32),
        in_specs=[smem, smem, smem, smem, vmem, vmem],
        out_specs=vmem,
        scratch_shapes=[
            pltpu.VMEM((relations * cells * rooms + 1, BLOCK, 128), jnp.bfloat16),
            pltpu.VMEM((2, BLOCK, 128), jnp.bfloat16),
            pltpu.VMEM((rows, slots + 128), jnp.float32),
            pltpu.VMEM((rows, slots + 128), jnp.float32),
        ],
        compiler_params=pltpu.CompilerParams(vmem_limit_bytes=56 * 1024 * 1024),
        name="density",
    )(block_list, chunks, counts.reshape(-1), jnp.sum(blocks, 1).reshape(-1), pos, padded.reshape(-1, 4, slots))
    return density.reshape(masses.shape)


def solution(mesh):
    in_specs = (
        P(None, "shear", None, "cross", None),
        P("shear", None, "cross", None),
        P("shear", None, "cross"),
        P(),
    )
    out_specs = P("shear", None, "cross", None)
    return jax.shard_map(shards, mesh=mesh, in_specs=in_specs, out_specs=out_specs, check_vma=False)
```
